128 devices in a mesh: ha: 4 (over z_lo, core), wa: 4 (over y), hd: 8 (over z_hi, x).
Axes of the slice: x: 4, y: 4, z: 4 (z_hi: 2, z_lo: 2; z = z_hi * 2 + z_lo), core: 2. Of those that a mesh axis runs over, the one named last changes fastest.
Arguments:
- queries: bfloat16 [12, 32, 64, 3072], P(None, 'ha', 'wa', 'hd'), may hold values from -10 to 10
- video_keys: bfloat16 [12, 32, 64, 3072], P(None, 'ha', 'wa', 'hd'), may hold values from -5 to 5
- video_values: bfloat16 [12, 32, 64, 3072], P(None, 'ha', 'wa', 'hd'), may hold values from -6 to 6
- text_keys: bfloat16 [256, 3072], P(None, 'hd'), may hold values from -5 to 5
- text_values: bfloat16 [256, 3072], P(None, 'hd'), may hold values from -6 to 6
- tile_radius: int32 [3, 2, 4, 8], P(None, None, 'ha', 'wa'), may hold values from 0 to 1, as said below
- out_weight: bfloat16 [3072, 3072], P('hd'), may hold values from -0.875 to 0.875
Outputs:
- projected: bfloat16 [12, 32, 64, 3072], P(None, 'ha', 'wa', 'hd')
The draws below stay inside these ranges and needn't reach their ends.
Inputs may be any that keep to these rules, and one draw needn't show every extreme that they name: `tile_radius`: every video query has a window of at most one tile in each direction; some tile has radius 1 in all three.
All inputs are finite; a program needn't handle non-finite values.
Results may differ from the reference program's by a relative error of at most 0.012.
Values may be sent and summed in bfloat16 or wider, within the bound.
No kernel may reach another device: no remote copies, remote signals or barrier semaphores. Data moves between devices by JAX's collectives and lax.ppermute only.
A program may use at most 192 MiB of HBM per device.

```python
import jax
import jax.numpy as jnp
from jax import lax

HEADS = 24
HEAD = 128
D = 3072
TEXT = 256
TILE_T = 6
TILE_H = 8
TILE_W = 8
TT_TILES = 2
FRAMES = 12
ROW_TILES = 4
COL_TILES = 8
HEIGHT = 32
WIDTH = 64
N_HD = 8


def paired_draw(key):
    base = jax.random.fold_in(key, 71)
    shape = (FRAMES, HEIGHT, WIDTH, HEADS * HEAD)
    first = jax.random.normal(jax.random.fold_in(base, 1), shape, jnp.float32)
    second = jax.random.normal(jax.random.fold_in(base, 2), shape, jnp.float32)
    q_part = jnp.clip(2.0 * first, -10.0, 10.0)
    k_part = jnp.clip(second, -5.0, 5.0)
    return (q_part, k_part)


def draw_queries(key, part):
    return paired_draw(key)[0].astype(jnp.bfloat16)


def draw_video_keys(key, part):
    return paired_draw(key)[1].astype(jnp.bfloat16)


def draw_tile_radius(key, part):
    drawn = jax.random.randint(key, (3, TT_TILES, ROW_TILES, COL_TILES), 0, 2).astype(jnp.int32)
    return drawn.at[:, 0, 0, 0].set(1)


def block_scale(key, extent, cuts, least, high):
    def one(dim, parts):
        draws = jax.random.uniform(jax.random.fold_in(jax.random.fold_in(key, 6), dim), (parts,), jnp.float32, least / len(cuts), high / len(cuts))
        return jnp.repeat(jnp.exp(draws), extent[dim] // parts).reshape((-1,) + (1,) * (len(extent) - dim - 1))

    factor_of = one(*cuts[0])
    for cut in cuts[1:]:
        factor_of = factor_of * one(*cut)
    return factor_of


def noise(key, shape, deviation, most, cuts=(), kind=jnp.bfloat16):
    values = jax.random.normal(key, shape, jnp.float32) * deviation
    if len(cuts) > 0:
        values = block_scale(key, shape, cuts, -0.22, 0.18) * values
    return jnp.clip(values, min=-most, max=most).astype(kind)


def setup_inputs(seed: int = 0) -> dict:
    key_of = jax.random.split(jax.random.key(seed), 8)
    return {
        "queries": draw_queries(jax.random.fold_in(key_of[7], 71), 0),
        "video_keys": draw_video_keys(jax.random.fold_in(key_of[7], 71), 0),
        "video_values": noise(key_of[2], (FRAMES, HEIGHT, WIDTH, HEADS * HEAD), 1.0, 6.0, ((1, 4), (2, 4), (3, 8))),
        "text_keys": noise(key_of[3], (TEXT, HEADS * HEAD), 1.0, 5.0, ((1, 8),)),
        "text_values": noise(key_of[4], (TEXT, HEADS * HEAD), 1.0, 6.0, ((1, 8),)),
        "tile_radius": draw_tile_radius(jax.random.fold_in(key_of[7], 71), 0),
        "out_weight": noise(key_of[6], (HEADS * HEAD, D), 48 ** -0.5, 0.875, ((0, 8),)),
    }


def reference(queries, video_keys, video_values, text_keys, text_values, tile_radius, out_weight):
    n_frames, n_height, n_width, channels = queries.shape
    time_tiles = n_frames // TILE_T
    row_tiles = n_height // TILE_H
    col_tiles = n_width // TILE_W
    head_count = channels // HEAD
    factor = HEAD ** -0.5
    padding = ((0, 0), (TILE_H, TILE_H), (TILE_W, TILE_W), (0, 0))
    keys_padded = jnp.pad(video_keys, padding)
    values_padded = jnp.pad(video_values, padding)
    text_key32 = text_keys.astype(jnp.float32).reshape(-1, head_count, HEAD)
    text_val32 = text_values.astype(jnp.float32).reshape(-1, head_count, HEAD)

    def one_tile(tile_index):
        time_tile = tile_index // (row_tiles * col_tiles)
        row_tile = (tile_index // col_tiles) % row_tiles
        col_tile = tile_index % col_tiles
        zero = jnp.zeros((), jnp.int32)
        q_tile = lax.dynamic_slice(queries, (time_tile * TILE_T, row_tile * TILE_H, col_tile * TILE_W, zero), (TILE_T, TILE_H, TILE_W, channels))
        q_tile = q_tile.astype(jnp.float32).reshape(-1, head_count, HEAD)
        k_tile = lax.dynamic_slice(keys_padded, (zero, row_tile * TILE_H, col_tile * TILE_W, zero), (n_frames, 3 * TILE_H, 3 * TILE_W, channels))
        v_tile = lax.dynamic_slice(values_padded, (zero, row_tile * TILE_H, col_tile * TILE_W, zero), (n_frames, 3 * TILE_H, 3 * TILE_W, channels))
        k_tile = k_tile.astype(jnp.float32).reshape(-1, head_count, HEAD)
        v_tile = v_tile.astype(jnp.float32).reshape(-1, head_count, HEAD)
        key_time = jnp.arange(n_frames, dtype=jnp.int32) // TILE_T
        key_row = row_tile - 1 + jnp.arange(3 * TILE_H, dtype=jnp.int32) // TILE_H
        key_col = col_tile - 1 + jnp.arange(3 * TILE_W, dtype=jnp.int32) // TILE_W
        radius_here = tile_radius[:, time_tile, row_tile, col_tile]
        time_ok = jnp.abs(key_time - time_tile) <= radius_here[0]
        row_ok = (jnp.abs(key_row - row_tile) <= radius_here[1]) & (key_row >= 0) & (key_row < row_tiles)
        col_ok = (jnp.abs(key_col - col_tile) <= radius_here[2]) & (key_col >= 0) & (key_col < col_tiles)
        allowed = (time_ok[:, None, None] & row_ok[None, :, None] & col_ok[None, None, :]).reshape(-1)
        scores = jnp.einsum("qhd,khd->hqk", q_tile, k_tile) * factor
        text_scores = jnp.einsum("qhd,khd->hqk", q_tile, text_key32) * factor
        row_peak = jnp.maximum(jnp.max(jnp.where(allowed[None, None, :], scores, -jnp.inf), axis=2), jnp.max(text_scores, axis=2))[:, :, None]
        weights = jnp.where(allowed[None, None, :], jnp.exp(scores - row_peak), 0.0)
        text_weights = jnp.exp(text_scores - row_peak)
        row_total = jnp.sum(weights, axis=2) + jnp.sum(text_weights, axis=2)
        weights_low = lax.optimization_barrier(weights.astype(jnp.bfloat16)).astype(jnp.float32)
        text_low = lax.optimization_barrier(text_weights.astype(jnp.bfloat16)).astype(jnp.float32)
        numerator = jnp.einsum("hqk,khd->qhd", weights_low, v_tile) + jnp.einsum("hqk,khd->qhd", text_low, text_val32)
        result = (numerator / jnp.transpose(row_total)[:, :, None]).astype(jnp.bfloat16)
        return result.reshape(TILE_T, TILE_H, TILE_W, channels)

    tiles = lax.map(one_tile, jnp.arange(time_tiles * row_tiles * col_tiles, dtype=jnp.int32))
    tiles = tiles.reshape(time_tiles, row_tiles, col_tiles, TILE_T, TILE_H, TILE_W, channels)
    attended = jnp.transpose(tiles, (0, 3, 1, 4, 2, 5, 6)).reshape(-1, channels)
    group_width = channels // N_HD
    summed = jnp.zeros((attended.shape[0], out_weight.shape[1]), jnp.float32)
    for group in range(N_HD):
        portion = jnp.dot(attended[:, group * group_width:(group + 1) * group_width], out_weight[group * group_width:(group + 1) * group_width], preferred_element_type=jnp.float32)
        summed = summed + lax.optimization_barrier(portion.astype(jnp.bfloat16)).astype(jnp.float32)
    return summed.astype(jnp.bfloat16).reshape(n_frames, n_height, n_width, -1)
```

```python
import functools
import jax
import jax.numpy as jnp
from jax import lax
from jax.experimental import pallas as pl
from jax.experimental.pallas import tpu as pltpu
from jax.sharding import PartitionSpec as P
HEAD=128; LIMIT=64.0
SCALE = 1.4426950408889634 * HEAD ** -0.5
NT=(((1,),(1,)),((),()))

def attend_kernel(rad, q, tk, tv, *refs, n_seg, coords, sub, QB):
    segs = refs[:n_seg]
    out = refs[n_seg:n_seg+2]
    qs, kbuf, vbuf, tvb, mref, peak, acc, lst, cnt, sems = refs[n_seg+2:]
    ha, wa, n_ha, n_wa = coords()
    copies=[]
    for i,s in enumerate(segs):
        copies.append(pltpu.make_async_copy(s.at[sub,0], kbuf.at[i], sems.at[2*i]))
        copies.append(pltpu.make_async_copy(s.at[sub,1], vbuf.at[i,:,pl.ds(0,128)], sems.at[2*i+1]))
    for c in copies: c.start()
    is_odd = ha % 2
    across_ok = jnp.where(is_odd==1, ha + 1 < n_ha, ha > 0).astype(jnp.int32)
    left_ok = (wa>0).astype(jnp.int32); right_ok=(wa+1<n_wa).astype(jnp.int32)
    rows=[0,0,1,1,2,2,0,0,1,1,2,2]
    cols=[0,1,0,1,0,1,-1,2,-1,2,-1,2]
    for t in range(2):
        for e in range(2):
            r0=rad[0,t,0,e]; r1=rad[1,t,0,e]; r2=rad[2,t,0,e]
            row_ok=[1, (r1>=1).astype(jnp.int32), jnp.where(r1>=1, across_ok, 0)]
            n=jnp.int32(0)
            for s in range(12):
                gap=abs(cols[s]-e)
                if gap>1: continue
                ok=row_ok[rows[s]]
                if gap==1: ok=ok*(r2>=1).astype(jnp.int32)
                if cols[s]==-1: ok=ok*left_ok
                if cols[s]==2: ok=ok*right_ok
                place=s
                if s in (4,5): place=4+abs(s-4-is_odd)
                if s in (10,11): place=11-is_odd if s==10 else 10+is_odd
                lst[2*t+e, n]=2*place+t
                n=n+ok
                lst[2*t+e, n]=2*place+1-t
                n=n+ok*(r0>=1).astype(jnp.int32)
            cnt[2*t+e]=n
    for t in range(2):
        for e in range(2):
            qs[2*t+e]=q[6*t:6*t+6,:,8*e:8*e+8,:].reshape(384,HEAD)
    ones=jnp.ones((768,128),jnp.bfloat16)
    def fill(s,_):
        vbuf[s,:,128:256]=ones
        return 0
    lax.fori_loop(0,12,fill,0)
    tvb[:,0:128]=tv[...]
    tvb[:,128:256]=jnp.ones((256,128),jnp.bfloat16)
    for c in copies: c.wait()

    def lanes_max(s):
        m=s[:,0:128]
        for j in range(1,s.shape[1]//128): m=jnp.maximum(m,s[:,128*j:128*j+128])
        return m
    def bc(m, w):
        return jnp.concatenate([m]*(w//128),axis=1)
    def one(qt,_):
        for r in range(0,384,QB):
            rs=pl.ds(r,QB)
            s=lax.dot_general(qs[qt,rs,:],tk[...],NT,preferred_element_type=jnp.float32)*SCALE
            m=jnp.broadcast_to(jnp.max(s,axis=1,keepdims=True),(QB,128))
            mref[rs,:]=m
            peak[rs,:]=m
            p=jnp.exp2(s-bc(m,256)).astype(jnp.bfloat16)
            acc[rs,:]=jnp.dot(p,tvb[...],preferred_element_type=jnp.float32)
        def block(i,_):
            idx=lst[qt,i]
            slot=idx//2; tt=idx%2
            ks=pl.ds(pl.multiple_of(tt*384,384),384)
            k=kbuf[slot,ks,:]; v=vbuf[slot,ks,:]
            for r in range(0,384,QB):
                rs=pl.ds(r,QB)
                s=lax.dot_general(qs[qt,rs,:],k,NT,preferred_element_type=jnp.float32)*SCALE
                peak[rs,:]=jnp.maximum(peak[rs,:],lanes_max(s))
                p=jnp.exp2(s-bc(mref[rs,:],384)).astype(jnp.bfloat16)
                acc[rs,:]+=jnp.dot(p,v,preferred_element_type=jnp.float32)
            return 0
        n=cnt[qt]
        lax.fori_loop(0,n,block,0)
        over=jnp.max(peak[...]-mref[...])
        @pl.when(over>LIMIT)
        def _():
            for r in range(0,384,128):
                rs=pl.ds(r,128)
                s=lax.dot_general(qs[qt,rs,:],tk[...],NT,preferred_element_type=jnp.float32)*SCALE
                p=jnp.exp2(s-bc(mref[rs,:],256)).astype(jnp.bfloat16)
                acc[rs,:]=jnp.dot(p,tvb[...],preferred_element_type=jnp.float32)
            def safe(i,_):
                idx=lst[qt,i]
                slot=idx//2; tt=idx%2
                ks=pl.ds(pl.multiple_of(tt*384,384),384)
                def part(j,_):
                    rs=pl.ds(pl.multiple_of(j*128,128),128)
                    s=lax.dot_general(qs[qt,rs,:],kbuf[slot,ks,:],NT,preferred_element_type=jnp.float32)*SCALE
                    old=mref[rs,:]
                    new=jnp.maximum(old,jnp.broadcast_to(jnp.max(s,axis=1,keepdims=True),(128,128)))
                    mref[rs,:]=new
                    p=jnp.exp2(s-bc(new,384)).astype(jnp.bfloat16)
                    acc[rs,:]=acc[rs,:]*bc(jnp.exp2(old-new),256)+jnp.dot(p,vbuf[slot,ks,:],preferred_element_type=jnp.float32)
                    return 0
                return lax.fori_loop(0,3,part,0)
            lax.fori_loop(0,n,safe,0)
        qs[qt]=(acc[:,0:128]/acc[:,128:256]).astype(jnp.bfloat16)
        return 0
    lax.fori_loop(0,4,one,0)
    for t in range(2):
        for e in range(2):
            out[t][:,:,8*e:8*e+8,:]=qs[2*t+e].reshape(6,8,8,HEAD)

def attend(rad,q,tk,tv,segs,h,sub,coords,QB=192):
    n=len(segs)
    return pl.pallas_call(
        functools.partial(attend_kernel,n_seg=n,coords=coords,sub=sub,QB=QB),
        grid=(1,),
        in_specs=[pl.BlockSpec(memory_space=pltpu.SMEM),
            pl.BlockSpec((12,8,16,HEAD),lambda i:(0,0,0,h)),
            pl.BlockSpec((256,HEAD),lambda i:(0,h)),
            pl.BlockSpec((256,HEAD),lambda i:(0,h))]+[pl.BlockSpec(memory_space=pl.ANY)]*n,
        out_specs=[pl.BlockSpec((6,8,16,HEAD),lambda i:(0,0,0,0))]*2,
        out_shape=[jax.ShapeDtypeStruct((6,8,16,HEAD),jnp.bfloat16)]*2,
        scratch_shapes=[pltpu.VMEM((4,384,HEAD),jnp.bfloat16),pltpu.VMEM((12,768,HEAD),jnp.bfloat16),
            pltpu.VMEM((12,768,256),jnp.bfloat16),pltpu.VMEM((256,256),jnp.bfloat16),
            pltpu.VMEM((384,128),jnp.float32),pltpu.VMEM((384,128),jnp.float32),pltpu.VMEM((384,256),jnp.float32),
            pltpu.SMEM((4,32),jnp.int32),pltpu.SMEM((4,),jnp.int32),pltpu.SemaphoreType.DMA((2*n,))],
        cost_estimate=pl.CostEstimate(flops=6_000_000_000,transcendentals=6_000_000,bytes_accessed=6_000_000),
        name="attend",
    )(rad,q,tk,tv,*segs)


GROUPS = ((0, 1), (1, 2))


def pack_kernel(*refs):
    low, high = refs[-2:]
    for i in range(low.shape[0]):
        for col, ref in enumerate((low, high)):
            for j in range(2):
                ref[i, j] = refs[2 * i + j][:, :, 8 * col : 8 * col + 8, :]


def pack(keys, values, first, count):
    specs = [
        pl.BlockSpec((12, 8, 16, HEAD), lambda i, h=h: (0, 0, 0, h))
        for h in range(first, first + count)
        for _ in range(2)
    ]
    shape = (count, 2, 12, 8, 8, HEAD)
    outs = pl.pallas_call(
        pack_kernel,
        grid=(1,),
        in_specs=specs,
        out_specs=[pl.BlockSpec(shape, lambda i: (0,) * 6)] * 2,
        out_shape=[jax.ShapeDtypeStruct(shape, jnp.bfloat16)] * 2,
        cost_estimate=pl.CostEstimate(flops=500_000_000, transcendentals=0, bytes_accessed=1_600_000),
        name="pack",
    )(*[keys, values] * count)
    return [out.reshape(count, 2, 768, HEAD) for out in outs]


def choose_kernel(own_low, own_high, partner_low, partner_high, out, sem):
    ha = lax.axis_index("ha")
    inner = (ha > 0) & (ha + 1 < lax.axis_size("ha"))
    odd = ha % 2 == 1
    for is_inner, refs in ((True, (own_low, own_high)), (False, (partner_low, partner_high))):
        for is_odd, ref in enumerate(refs):

            @pl.when((inner == is_inner) & (odd == bool(is_odd)))
            def _():
                copy = pltpu.make_async_copy(ref, out, sem)
                copy.start()
                copy.wait()


def choose(*pieces):
    return pl.pallas_call(
        choose_kernel,
        in_specs=[pl.BlockSpec(memory_space=pl.ANY)] * 4,
        out_shape=jax.ShapeDtypeStruct(pieces[0].shape, jnp.bfloat16),
        scratch_shapes=[pltpu.SemaphoreType.DMA],
        cost_estimate=pl.CostEstimate(flops=200_000_000, transcendentals=0, bytes_accessed=800_000),
        name="choose",
    )(*pieces)


def cut_kernel(w, own, plus, minus, far):
    hd = lax.axis_index("hd")
    x = hd % 4
    plane = hd // 4
    for ref, step in ((own, 0), (plus, 1), (minus, 3), (far, 2)):
        for j in range(2):
            col = (x + step) % 4 + 4 * ((plane + j) % 2)
            ref[j] = w[:, pl.ds(pl.multiple_of(col * 384, 384), 384)]


def cut(weight):
    return pl.pallas_call(
        cut_kernel,
        out_shape=[jax.ShapeDtypeStruct((2, 384, 384), jnp.bfloat16)] * 4,
        cost_estimate=pl.CostEstimate(flops=500_000_000, transcendentals=0, bytes_accessed=4_800_000),
        name="cut",
    )(weight)


def project_kernel(*refs):
    rows = refs[:12]
    weights = refs[12:16]
    mine, other, a, b = refs[16:]
    for i in range(12):
        a[:, HEAD * i : HEAD * (i + 1)] = rows[i][...].reshape(768, HEAD)
    for i in range(4):
        for j in range(2):
            b[384 * i : 384 * (i + 1), 384 * j : 384 * (j + 1)] = weights[i][j]
    other[...] = (
        jnp.dot(a[...], b[:, 384:768], preferred_element_type=jnp.float32)
        .astype(jnp.bfloat16)
        .reshape(6, 8, 16, 384)
    )
    mine[...] = jnp.dot(a[...], b[:, 0:384], preferred_element_type=jnp.float32).reshape(6, 8, 16, 384)


def project(rows, weights):
    return pl.pallas_call(
        project_kernel,
        out_shape=[
            jax.ShapeDtypeStruct((6, 8, 16, 384), jnp.float32),
            jax.ShapeDtypeStruct((6, 8, 16, 384), jnp.bfloat16),
        ],
        scratch_shapes=[pltpu.VMEM((768, 1536), jnp.bfloat16), pltpu.VMEM((1536, 768), jnp.bfloat16)],
        cost_estimate=pl.CostEstimate(flops=2_000_000_000, transcendentals=0, bytes_accessed=9_000_000),
        name="project",
    )(*rows, *weights)


def hd_pairs(step, planes=0):
    return [
        (4 * z + x, 4 * ((z + planes) % 2) + (x + step) % 4) for z in range(2) for x in range(4)
    ]


def place():
    return lax.axis_index("ha"), lax.axis_index("wa"), lax.axis_size("ha"), lax.axis_size("wa")


def shards(queries, video_keys, video_values, text_keys, text_values, tile_radius, out_weight):
    n_ha = lax.axis_size("ha")
    n_wa = lax.axis_size("wa")
    ring = [(i, (i + 1) % n_wa) for i in range(n_wa)]
    back = [(t, s) for s, t in ring]
    partner = [(i, i + 1 if i % 2 == 0 else i - 1) for i in range(n_ha)]
    chips = [(i, (i + 2) % n_ha) for i in range(n_ha)]
    turn = [
        (i * n_wa + s, i * n_wa + t)
        for i in range(n_ha)
        for s, t in (ring if i % 2 else back)
    ]

    def swap(piece):
        return lax.ppermute(piece, "ha", partner)

    windows = []
    for first, count in GROUPS:
        low, high = pack(video_keys, video_values, first, count)
        from_left = lax.ppermute(high, "wa", ring)
        from_right = lax.ppermute(low, "wa", back)
        partner_low, partner_high = swap(low), swap(high)
        over = lax.ppermute(choose(low, high, partner_low, partner_high), "ha", chips)
        corner = lax.ppermute(over, ("ha", "wa"), turn)
        window = (low, high, partner_low, partner_high, over, swap(over), from_left, from_right,
                  swap(from_left), swap(from_right), corner, swap(corner))
        windows += [(window, i) for i in range(count)]
    pieces = cut(out_weight)
    weights = [
        pieces[0],
        lax.ppermute(pieces[1], "hd", hd_pairs(1)),
        lax.ppermute(pieces[2], "hd", hd_pairs(-1)),
        lax.ppermute(pieces[3], "hd", hd_pairs(2)),
    ]
    rows = [[], []]
    for h in range(3):
        halves = attend(tile_radius, queries, text_keys, text_values, windows[h][0], h, windows[h][1], place)
        for t in range(2):
            forward = lax.ppermute(halves[t], "hd", hd_pairs(1))
            backward = lax.ppermute(halves[t], "hd", hd_pairs(-1))
            if t == 0:
                far = lax.ppermute(forward, "hd", hd_pairs(1))
            else:
                far = lax.ppermute(backward, "hd", hd_pairs(-1))
            rows[t].append((halves[t], forward, backward, far))
    outs = []
    for t in range(2):
        mine, other = project([rows[t][h][g] for g in range(4) for h in range(3)], weights)
        arrived = lax.ppermute(other, "hd", hd_pairs(0, 1))
        outs.append((mine + arrived.astype(jnp.float32)).astype(jnp.bfloat16))
    return jnp.concatenate(outs, axis=0)


def solution(mesh):
    placed = (
        P(None, "ha", "wa", "hd"),
        P(None, "ha", "wa", "hd"),
        P(None, "ha", "wa", "hd"),
        P(None, "hd"),
        P(None, "hd"),
        P(None, None, "ha", "wa"),
        P("hd", None),
    )
    return jax.shard_map(
        shards, mesh=mesh, in_specs=placed, out_specs=P(None, "ha", "wa", "hd"), check_vma=False
    )
```

```python
import functools
import jax
import jax.numpy as jnp
from jax import lax
from jax.experimental import pallas as pl
from jax.experimental.pallas import tpu as pltpu
from jax.sharding import PartitionSpec as P

HEAD=128; LIMIT=64.0
SCALE = 1.4426950408889634 * HEAD ** -0.5
NT=(((1,),(1,)),((),()))


def attend_kernel(rad, q, tk, tv, *refs, n_seg, coords, sub, times, split, QB):
    segs = refs[:n_seg]
    qs, kbuf, vbuf, tvb, mref, peak, acc, lst, cnt, sems = refs[-10:]
    out = refs[n_seg:-10]
    tiles = [(t, e) for t in times for e in range(2)]
    base = 6 * times[0]
    ha, wa, n_ha, n_wa = coords()
    copies=[]
    for i,s in enumerate(segs):
        copies.append(pltpu.make_async_copy(s.at[sub,0], kbuf.at[i], sems.at[2*i]))
        copies.append(pltpu.make_async_copy(s.at[sub,1], vbuf.at[i,:,pl.ds(0,128)], sems.at[2*i+1]))
    for c in copies: c.start()
    is_odd = ha % 2
    across_ok = jnp.where(is_odd==1, ha + 1 < n_ha, ha > 0).astype(jnp.int32)
    left_ok = (wa>0).astype(jnp.int32); right_ok=(wa+1<n_wa).astype(jnp.int32)
    rows=[0,0,1,1,2,2,0,0,1,1,2,2]
    cols=[0,1,0,1,0,1,-1,2,-1,2,-1,2]
    for qt, (t, e) in enumerate(tiles):
        r0=rad[0,t,0,e]; r1=rad[1,t,0,e]; r2=rad[2,t,0,e]
        row_ok=[1, (r1>=1).astype(jnp.int32), jnp.where(r1>=1, across_ok, 0)]
        n=jnp.int32(0)
        for s in range(12):
            gap=abs(cols[s]-e)
            if gap>1: continue
            ok=row_ok[rows[s]]
            if gap==1: ok=ok*(r2>=1).astype(jnp.int32)
            if cols[s]==-1: ok=ok*left_ok
            if cols[s]==2: ok=ok*right_ok
            place=s
            if s in (4,5): place=4+abs(s-4-is_odd)
            if s in (10,11): place=11-is_odd if s==10 else 10+is_odd
            lst[qt, n]=2*place+t
            n=n+ok
            lst[qt, n]=2*place+1-t
            n=n+ok*(r0>=1).astype(jnp.int32)
        cnt[qt]=n
    for qt, (t, e) in enumerate(tiles):
        f=6*t-base
        qs[qt]=q[f:f+6,:,8*e:8*e+8,:].reshape(384,HEAD)
    ones=jnp.ones((768,128),jnp.bfloat16)
    def fill(s,_):
        vbuf[s,:,128:256]=ones
        return 0
    lax.fori_loop(0,12,fill,0)
    tvb[:,0:128]=tv[...]
    tvb[:,128:256]=jnp.ones((256,128),jnp.bfloat16)

    def lanes_max(s):
        m=[s[:,128*j:128*j+128] for j in range(s.shape[1]//128)]
        while len(m)>1: m=[jnp.maximum(a,b) for a,b in zip(m[::2],m[1::2])]+([m[-1]] if len(m)%2 else [])
        return m[0]
    def bc(m, w):
        return jnp.concatenate([m]*(w//128),axis=1)
    def scores(qv,k):
        return lax.dot_general(qv,k,NT,preferred_element_type=jnp.float32)*SCALE
    def keys(code):
        return code//2, pl.ds(pl.multiple_of((code%2)*384,384),384)
    def text(qt,track):
        for r in range(0,384,QB):
            rs=pl.ds(r,QB)
            s=scores(qs[qt,rs,:],tk[...])
            if track:
                m=jnp.broadcast_to(jnp.max(s,axis=1,keepdims=True),(QB,128))
                mref[qt,rs,:]=m
                peak[qt,rs,:]=m
            else:
                m=mref[qt,rs,:]
            p=jnp.exp2(s-bc(m,256)).astype(jnp.bfloat16)
            acc[qt,rs,:]=jnp.dot(p,tvb[...],preferred_element_type=jnp.float32)
    def step(qt,codes):
        at=[keys(c) for c in codes]
        k=jnp.concatenate([kbuf[s,ks,:] for s,ks in at],axis=0)
        v=jnp.concatenate([vbuf[s,ks,:] for s,ks in at],axis=0)
        nxt=scores(qs[qt,pl.ds(0,QB),:],k)
        for r in range(0,384,QB):
            s=nxt
            if r+QB<384: nxt=scores(qs[qt,pl.ds(r+QB,QB),:],k)
            rs=pl.ds(r,QB)
            peak[qt,rs,:]=jnp.maximum(peak[qt,rs,:],lanes_max(s))
            p=jnp.exp2(s-bc(mref[qt,rs,:],s.shape[1])).astype(jnp.bfloat16)
            acc[qt,rs,:]+=jnp.dot(p,v,preferred_element_type=jnp.float32)
    for qt in range(len(tiles)):
        text(qt,True)
    for c in copies: c.wait()
    def one(qt,_):
        n=cnt[qt]
        def pair(i,_):
            step(qt,(lst[qt,2*i],lst[qt,2*i+1]))
            return 0
        lax.fori_loop(0,n//2,pair,0)
        @pl.when(n%2==1)
        def _():
            step(qt,(lst[qt,n-1],))
        return 0
    lax.fori_loop(0,len(tiles),one,0)
    gap=peak[0]-mref[0]
    for qt in range(1,len(tiles)): gap=jnp.maximum(gap,peak[qt]-mref[qt])
    @pl.when(jnp.max(gap)>LIMIT)
    def _():
        def redo(qt,_):
            text(qt,False)
            def safe(i,_):
                slot,ks=keys(lst[qt,i])
                def part(j,_):
                    rs=pl.ds(pl.multiple_of(j*128,128),128)
                    s=scores(qs[qt,rs,:],kbuf[slot,ks,:])
                    old=mref[qt,rs,:]
                    new=jnp.maximum(old,jnp.broadcast_to(jnp.max(s,axis=1,keepdims=True),(128,128)))
                    mref[qt,rs,:]=new
                    p=jnp.exp2(s-bc(new,384)).astype(jnp.bfloat16)
                    acc[qt,rs,:]=acc[qt,rs,:]*bc(jnp.exp2(old-new),256)+jnp.dot(p,vbuf[slot,ks,:],preferred_element_type=jnp.float32)
                    return 0
                return lax.fori_loop(0,3,part,0)
            return lax.fori_loop(0,cnt[qt],safe,0)
        lax.fori_loop(0,len(tiles),redo,0)
    for qt, (t, e) in enumerate(tiles):
        ref=out[times.index(t) if split else 0]
        f=0 if split else 6*t-base
        ref[f:f+6,:,8*e:8*e+8,:]=(acc[qt,:,0:128]/acc[qt,:,128:256]).astype(jnp.bfloat16).reshape(6,8,8,HEAD)


def attend(rad,q,tk,tv,segs,h,sub,coords,times=(0,1),split=True,QB=192):
    n=len(segs); nt=2*len(times); frames=6*len(times)
    first=times[0] if len(times)==1 else 0
    size=6 if split else frames
    return pl.pallas_call(
        functools.partial(attend_kernel,n_seg=n,coords=coords,sub=sub,times=times,split=split,QB=QB),
        grid=(1,),
        in_specs=[pl.BlockSpec(memory_space=pltpu.SMEM),
            pl.BlockSpec((frames,8,16,HEAD),lambda i:(first,0,0,h)),
            pl.BlockSpec((256,HEAD),lambda i:(0,h)),
            pl.BlockSpec((256,HEAD),lambda i:(0,h))]+[pl.BlockSpec(memory_space=pltpu.HBM)]*n,
        out_specs=[pl.BlockSpec((size,8,16,HEAD),lambda i:(0,0,0,0))]*(frames//size),
        out_shape=[jax.ShapeDtypeStruct((size,8,16,HEAD),jnp.bfloat16)]*(frames//size),
        scratch_shapes=[pltpu.VMEM((nt,384,HEAD),jnp.bfloat16),pltpu.VMEM((12,768,HEAD),jnp.bfloat16),
            pltpu.VMEM((12,768,256),jnp.bfloat16),pltpu.VMEM((256,256),jnp.bfloat16),
            pltpu.VMEM((nt,384,128),jnp.float32),pltpu.VMEM((nt,384,128),jnp.float32),pltpu.VMEM((nt,384,256),jnp.float32),
            pltpu.SMEM((nt,32),jnp.int32),pltpu.SMEM((nt,),jnp.int32),pltpu.SemaphoreType.DMA((2*n,))],
        cost_estimate=pl.CostEstimate(flops=3_000_000_000*len(times),transcendentals=6_000_000,bytes_accessed=6_000_000),
        name="attend",
    )(rad,q,tk,tv,*segs)


GROUPS = ((0, 1), (1, 2))


def pack_kernel(*refs):
    low, high = refs[-2:]
    for i in range(low.shape[0]):
        for col, ref in enumerate((low, high)):
            for j in range(2):
                ref[i, j] = refs[2 * i + j][:, :, 8 * col : 8 * col + 8, :]


def pack(keys, values, first, count):
    specs = [
        pl.BlockSpec((12, 8, 16, HEAD), lambda i, h=h: (0, 0, 0, h))
        for h in range(first, first + count)
        for _ in range(2)
    ]
    shape = (count, 2, 12, 8, 8, HEAD)
    outs = pl.pallas_call(
        pack_kernel,
        grid=(1,),
        in_specs=specs,
        out_specs=[pl.BlockSpec(shape, lambda i: (0,) * 6)] * 2,
        out_shape=[jax.ShapeDtypeStruct(shape, jnp.bfloat16)] * 2,
        cost_estimate=pl.CostEstimate(flops=500_000_000, transcendentals=0, bytes_accessed=1_600_000),
        name="pack",
    )(*[keys, values] * count)
    return [out.reshape(count, 2, 768, HEAD) for out in outs]


def choose_kernel(own_low, own_high, partner_low, partner_high, out, sem):
    ha = lax.axis_index("ha")
    inner = (ha > 0) & (ha + 1 < lax.axis_size("ha"))
    odd = ha % 2 == 1
    for is_inner, refs in ((True, (own_low, own_high)), (False, (partner_low, partner_high))):
        for is_odd, ref in enumerate(refs):

            @pl.when((inner == is_inner) & (odd == bool(is_odd)))
            def _():
                copy = pltpu.make_async_copy(ref, out, sem)
                copy.start()
                copy.wait()


def choose(*pieces):
    return pl.pallas_call(
        choose_kernel,
        in_specs=[pl.BlockSpec(memory_space=pltpu.HBM)] * 4,
        out_shape=jax.ShapeDtypeStruct(pieces[0].shape, jnp.bfloat16),
        scratch_shapes=[pltpu.SemaphoreType.DMA],
        cost_estimate=pl.CostEstimate(flops=200_000_000, transcendentals=0, bytes_accessed=800_000),
        name="choose",
    )(*pieces)


def cut_kernel(w, own, plus, minus, far):
    hd = lax.axis_index("hd")
    x = hd % 4
    plane = hd // 4
    for ref, step in ((own, 0), (plus, 1), (minus, 3), (far, 2)):
        for j in range(2):
            col = (x + step) % 4 + 4 * ((plane + j) % 2)
            ref[j] = w[:, pl.ds(pl.multiple_of(col * 384, 384), 384)]


def cut(weight):
    return pl.pallas_call(
        cut_kernel,
        out_shape=[jax.ShapeDtypeStruct((2, 384, 384), jnp.bfloat16)] * 4,
        cost_estimate=pl.CostEstimate(flops=500_000_000, transcendentals=0, bytes_accessed=4_800_000),
        name="cut",
    )(weight)


def product(refs, weights, a, b):
    @pl.when(pl.program_id(0) == 0)
    def _():
        for i in range(4):
            b[384 * i : 384 * (i + 1), :] = weights[i][0]

    for i in range(12):
        a[:, HEAD * i : HEAD * (i + 1)] = refs[i][...].reshape(256, HEAD)
    return jnp.dot(a[...], b[...], preferred_element_type=jnp.float32).reshape(2, 8, 16, 384)


def project_kernel(*refs):
    out, a, b = refs[16:]
    out[...] = product(refs, refs[12:16], a, b).astype(out.dtype)


def project(rows, weights, half, side, dtype):
    specs = [
        pl.BlockSpec((2, 8, 16, HEAD), lambda i, f=3 * half * (r.shape[0] // 12): (f + i, 0, 0, 0))
        for r in rows
    ]
    return pl.pallas_call(
        project_kernel,
        grid=(3,),
        in_specs=specs + [pl.BlockSpec((1, 384, 384), lambda i: (side, 0, 0))] * 4,
        out_specs=pl.BlockSpec((2, 8, 16, 384), lambda i: (i, 0, 0, 0)),
        out_shape=jax.ShapeDtypeStruct((6, 8, 16, 384), dtype),
        scratch_shapes=[pltpu.VMEM((256, 1536), jnp.bfloat16), pltpu.VMEM((1536, 384), jnp.bfloat16)],
        cost_estimate=pl.CostEstimate(flops=1_000_000_000, transcendentals=0, bytes_accessed=4_500_000),
        name="project",
    )(*rows, *weights)


def hd_pairs(step, planes=0):
    return [
        (4 * z + x, 4 * ((z + planes) % 2) + (x + step) % 4) for z in range(2) for x in range(4)
    ]


def place():
    return lax.axis_index("ha"), lax.axis_index("wa"), lax.axis_size("ha"), lax.axis_size("wa")


def shards(queries, video_keys, video_values, text_keys, text_values, tile_radius, out_weight):
    n_ha = lax.axis_size("ha")
    n_wa = lax.axis_size("wa")
    ring = [(i, (i + 1) % n_wa) for i in range(n_wa)]
    back = [(t, s) for s, t in ring]
    partner = [(i, i + 1 if i % 2 == 0 else i - 1) for i in range(n_ha)]
    chips = [(i, (i + 2) % n_ha) for i in range(n_ha)]
    turn = [
        (i * n_wa + s, i * n_wa + t)
        for i in range(n_ha)
        for s, t in (ring if i % 2 else back)
    ]

    def swap(piece):
        return lax.ppermute(piece, "ha", partner)

    windows = []
    for first, count in GROUPS:
        low, high = pack(video_keys, video_values, first, count)
        from_left = lax.ppermute(high, "wa", ring)
        from_right = lax.ppermute(low, "wa", back)
        partner_low, partner_high = swap(low), swap(high)
        picked = choose(low, high, partner_low, partner_high)
        over = lax.ppermute(picked, "ha", chips)
        corner = lax.ppermute(over, ("ha", "wa"), turn)
        window = (low, high, partner_low, partner_high, over, swap(over),
                  from_left, from_right, swap(from_left), swap(from_right),
                  corner, swap(corner))
        windows += [(window, i) for i in range(count)]
    pieces = cut(out_weight)
    weights = [
        pieces[0],
        lax.ppermute(pieces[1], "hd", hd_pairs(1)),
        lax.ppermute(pieces[2], "hd", hd_pairs(-1)),
        lax.ppermute(pieces[3], "hd", hd_pairs(2)),
    ]
    def spread(piece):
        return [
            piece,
            lax.ppermute(piece, "hd", hd_pairs(1)),
            lax.ppermute(piece, "hd", hd_pairs(-1)),
            lax.ppermute(piece, "hd", hd_pairs(2)),
        ]

    def head(h, times, split):
        window, sub = windows[h]
        return attend(tile_radius, queries, text_keys, text_values, window, h, sub, place, times, split)

    (whole,) = head(0, (0, 1), False)
    gathered = [[spread(whole)] * 2]
    halves = head(1, (0, 1), True)
    gathered.append([spread(halves[t]) for t in range(2)])
    last = {t: spread(head(2, (t,), True)[0]) for t in (1, 0)}
    gathered.append([last[0], last[1]])
    lines = [[gathered[h][t][g] for g in range(4) for h in range(3)] for t in range(2)]
    arrived = {}
    for t in (1, 0):
        other = project(lines[t], weights, t, 1, jnp.bfloat16)
        arrived[t] = lax.ppermute(other, "hd", hd_pairs(0, 1))
    outs = []
    for t in range(2):
        mine = project(lines[t], weights, t, 0, jnp.float32)
        outs.append((mine + arrived[t].astype(jnp.float32)).astype(jnp.bfloat16))
    return jnp.concatenate(outs, axis=0)


def solution(mesh):
    placed = (
        P(None, "ha", "wa", "hd"),
        P(None, "ha", "wa", "hd"),
        P(None, "ha", "wa", "hd"),
        P(None, "hd"),
        P(None, "hd"),
        P(None, None, "ha", "wa"),
        P("hd", None),
    )
    return jax.shard_map(
        shards, mesh=mesh, in_specs=placed, out_specs=P(None, "ha", "wa", "hd"), check_vma=False
    )
```

```python
import functools
import jax
import jax.numpy as jnp
from jax import lax
from jax.experimental import pallas as pl
from jax.experimental.pallas import tpu as pltpu
from jax.sharding import PartitionSpec as P

HEAD=128; LIMIT=64.0
SCALE = 1.4426950408889634 * HEAD ** -0.5
NT=(((1,),(1,)),((),()))


def attend_kernel(rad, q, tk, tv, *refs, n_seg, coords, sub, times, split, QB):
    segs = refs[:n_seg]
    qs, kbuf, vbuf, tvb, mref, peak, acc, lst, cnt, sems = refs[-10:]
    out = refs[n_seg:-10]
    tiles = [(t, e) for t in times for e in range(2)]
    base = 6 * times[0]
    ha, wa, n_ha, n_wa = coords()
    copies=[]
    for i,s in enumerate(segs):
        copies.append(pltpu.make_async_copy(s.at[sub,0], kbuf.at[i], sems.at[2*i]))
        copies.append(pltpu.make_async_copy(s.at[sub,1], vbuf.at[i,:,pl.ds(0,128)], sems.at[2*i+1]))
    for c in copies: c.start()
    is_odd = ha % 2
    across_ok = jnp.where(is_odd==1, ha + 1 < n_ha, ha > 0).astype(jnp.int32)
    left_ok = (wa>0).astype(jnp.int32); right_ok=(wa+1<n_wa).astype(jnp.int32)
    rows=[0,0,1,1,2,2,0,0,1,1,2,2]
    cols=[0,1,0,1,0,1,-1,2,-1,2,-1,2]
    for qt, (t, e) in enumerate(tiles):
        r0=rad[0,t,0,e]; r1=rad[1,t,0,e]; r2=rad[2,t,0,e]
        row_ok=[1, (r1>=1).astype(jnp.int32), jnp.where(r1>=1, across_ok, 0)]
        n=jnp.int32(0)
        for s in range(12):
            gap=abs(cols[s]-e)
            if gap>1: continue
            ok=row_ok[rows[s]]
            if gap==1: ok=ok*(r2>=1).astype(jnp.int32)
            if cols[s]==-1: ok=ok*left_ok
            if cols[s]==2: ok=ok*right_ok
            place=s
            if s in (4,5): place=4+abs(s-4-is_odd)
            if s in (10,11): place=11-is_odd if s==10 else 10+is_odd
            lst[qt, n]=2*place+t
            n=n+ok
            lst[qt, n]=2*place+1-t
            n=n+ok*(r0>=1).astype(jnp.int32)
        cnt[qt]=n
    for qt, (t, e) in enumerate(tiles):
        f=6*t-base
        qs[qt]=q[f:f+6,:,8*e:8*e+8,:].reshape(384,HEAD)
    ones=jnp.ones((768,128),jnp.bfloat16)
    def fill(s,_):
        vbuf[s,:,128:256]=ones
        return 0
    lax.fori_loop(0,12,fill,0)
    tvb[:,0:128]=tv[...]
    tvb[:,128:256]=jnp.ones((256,128),jnp.bfloat16)

    def lanes_max(s):
        m=[s[:,128*j:128*j+128] for j in range(s.shape[1]//128)]
        while len(m)>1: m=[jnp.maximum(a,b) for a,b in zip(m[::2],m[1::2])]+([m[-1]] if len(m)%2 else [])
        return m[0]
    def bc(m, w):
        return jnp.concatenate([m]*(w//128),axis=1)
    def scores(qv,k):
        return lax.dot_general(qv,k,NT,preferred_element_type=jnp.float32)*SCALE
    def keys(code):
        return code//2, pl.ds(pl.multiple_of((code%2)*384,384),384)
    def text(qt,track):
        for r in range(0,384,QB):
            rs=pl.ds(r,QB)
            s=scores(qs[qt,rs,:],tk[...])
            if track:
                m=jnp.broadcast_to(jnp.max(s,axis=1,keepdims=True),(QB,128))
                mref[qt,rs,:]=m
                peak[qt,rs,:]=m
            else:
                m=mref[qt,rs,:]
            p=jnp.exp2(s-bc(m,256)).astype(jnp.bfloat16)
            acc[qt,rs,:]=jnp.dot(p,tvb[...],preferred_element_type=jnp.float32)
    def step(qt,codes):
        at=[keys(c) for c in codes]
        k=jnp.concatenate([kbuf[s,ks,:] for s,ks in at],axis=0)
        v=jnp.concatenate([vbuf[s,ks,:] for s,ks in at],axis=0)
        nxt=scores(qs[qt,pl.ds(0,QB),:],k)
        for r in range(0,384,QB):
            s=nxt
            if r+QB<384: nxt=scores(qs[qt,pl.ds(r+QB,QB),:],k)
            rs=pl.ds(r,QB)
            peak[qt,rs,:]=jnp.maximum(peak[qt,rs,:],lanes_max(s))
            p=jnp.exp2(s-bc(mref[qt,rs,:],s.shape[1])).astype(jnp.bfloat16)
            acc[qt,rs,:]+=jnp.dot(p,v,preferred_element_type=jnp.float32)
    for qt in range(len(tiles)):
        text(qt,True)
    for c in copies: c.wait()
    def one(qt,_):
        n=cnt[qt]
        def pair(i,_):
            step(qt,(lst[qt,2*i],lst[qt,2*i+1]))
            return 0
        lax.fori_loop(0,n//2,pair,0)
        @pl.when(n%2==1)
        def _():
            step(qt,(lst[qt,n-1],))
        return 0
    lax.fori_loop(0,len(tiles),one,0)
    gap=peak[0]-mref[0]
    for qt in range(1,len(tiles)): gap=jnp.maximum(gap,peak[qt]-mref[qt])
    @pl.when(jnp.max(gap)>LIMIT)
    def _():
        def redo(qt,_):
            text(qt,False)
            def safe(i,_):
                slot,ks=keys(lst[qt,i])
                def part(j,_):
                    rs=pl.ds(pl.multiple_of(j*128,128),128)
                    s=scores(qs[qt,rs,:],kbuf[slot,ks,:])
                    old=mref[qt,rs,:]
                    new=jnp.maximum(old,jnp.broadcast_to(jnp.max(s,axis=1,keepdims=True),(128,128)))
                    mref[qt,rs,:]=new
                    p=jnp.exp2(s-bc(new,384)).astype(jnp.bfloat16)
                    acc[qt,rs,:]=acc[qt,rs,:]*bc(jnp.exp2(old-new),256)+jnp.dot(p,vbuf[slot,ks,:],preferred_element_type=jnp.float32)
                    return 0
                return lax.fori_loop(0,3,part,0)
            return lax.fori_loop(0,cnt[qt],safe,0)
        lax.fori_loop(0,len(tiles),redo,0)
    for qt, (t, e) in enumerate(tiles):
        ref=out[times.index(t) if split else 0]
        f=0 if split else 6*t-base
        ref[f:f+6,:,8*e:8*e+8,:]=(acc[qt,:,0:128]/acc[qt,:,128:256]).astype(jnp.bfloat16).reshape(6,8,8,HEAD)


def attend(rad,q,tk,tv,segs,h,sub,coords,times=(0,1),split=True,QB=192):
    n=len(segs); nt=2*len(times); frames=6*len(times)
    first=times[0] if len(times)==1 else 0
    size=6 if split else frames
    return pl.pallas_call(
        functools.partial(attend_kernel,n_seg=n,coords=coords,sub=sub,times=times,split=split,QB=QB),
        grid=(1,),
        in_specs=[pl.BlockSpec(memory_space=pltpu.SMEM),
            pl.BlockSpec((frames,8,16,HEAD),lambda i:(first,0,0,h)),
            pl.BlockSpec((256,HEAD),lambda i:(0,h)),
            pl.BlockSpec((256,HEAD),lambda i:(0,h))]+[pl.BlockSpec(memory_space=pltpu.HBM)]*n,
        out_specs=[pl.BlockSpec((size,8,16,HEAD),lambda i:(0,0,0,0))]*(frames//size),
        out_shape=[jax.ShapeDtypeStruct((size,8,16,HEAD),jnp.bfloat16)]*(frames//size),
        scratch_shapes=[pltpu.VMEM((nt,384,HEAD),jnp.bfloat16),pltpu.VMEM((12,768,HEAD),jnp.bfloat16),
            pltpu.VMEM((12,768,256),jnp.bfloat16),pltpu.VMEM((256,256),jnp.bfloat16),
            pltpu.VMEM((nt,384,128),jnp.float32),pltpu.VMEM((nt,384,128),jnp.float32),pltpu.VMEM((nt,384,256),jnp.float32),
            pltpu.SMEM((nt,32),jnp.int32),pltpu.SMEM((nt,),jnp.int32),pltpu.SemaphoreType.DMA((2*n,))],
        cost_estimate=pl.CostEstimate(flops=3_000_000_000*len(times),transcendentals=6_000_000,bytes_accessed=6_000_000),
        name="attend",
    )(rad,q,tk,tv,*segs)


GROUPS = ((0, 1), (1, 2))
STEPS = 1


def pack_kernel(*refs):
    low, high = refs[-2:]
    for i in range(low.shape[0]):
        for col, ref in enumerate((low, high)):
            for j in range(2):
                ref[i, j] = refs[2 * i + j][:, :, 8 * col : 8 * col + 8, :]


def pack(keys, values, first, count):
    specs = [
        pl.BlockSpec((12, 8, 16, HEAD), lambda i, h=h: (0, 0, 0, h))
        for h in range(first, first + count)
        for _ in range(2)
    ]
    shape = (count, 2, 12, 8, 8, HEAD)
    outs = pl.pallas_call(
        pack_kernel,
        grid=(1,),
        in_specs=specs,
        out_specs=[pl.BlockSpec(shape, lambda i: (0,) * 6)] * 2,
        out_shape=[jax.ShapeDtypeStruct(shape, jnp.bfloat16)] * 2,
        cost_estimate=pl.CostEstimate(flops=500_000_000, transcendentals=0, bytes_accessed=1_600_000),
        name="pack",
    )(*[keys, values] * count)
    return [out.reshape(count, 2, 768, HEAD) for out in outs]


def choose_kernel(own_low, own_high, partner_low, partner_high, out, sem):
    ha = lax.axis_index("ha")
    inner = (ha > 0) & (ha + 1 < lax.axis_size("ha"))
    odd = ha % 2 == 1
    for is_inner, refs in ((True, (own_low, own_high)), (False, (partner_low, partner_high))):
        for is_odd, ref in enumerate(refs):

            @pl.when((inner == is_inner) & (odd == bool(is_odd)))
            def _():
                copy = pltpu.make_async_copy(ref, out, sem)
                copy.start()
                copy.wait()


def choose(*pieces):
    return pl.pallas_call(
        choose_kernel,
        in_specs=[pl.BlockSpec(memory_space=pltpu.HBM)] * 4,
        out_shape=jax.ShapeDtypeStruct(pieces[0].shape, jnp.bfloat16),
        scratch_shapes=[pltpu.SemaphoreType.DMA],
        cost_estimate=pl.CostEstimate(flops=200_000_000, transcendentals=0, bytes_accessed=800_000),
        name="choose",
    )(*pieces)


def cut_kernel(w, own, plus, minus, far):
    hd = lax.axis_index("hd")
    x = hd % 4
    plane = hd // 4
    for ref, step in ((own, 0), (plus, 1), (minus, 3), (far, 2)):
        for j in range(2):
            col = (x + step) % 4 + 4 * ((plane + j) % 2)
            ref[j] = w[:, pl.ds(pl.multiple_of(col * 384, 384), 384)]


def cut(weight):
    return pl.pallas_call(
        cut_kernel,
        out_shape=[jax.ShapeDtypeStruct((2, 384, 384), jnp.bfloat16)] * 4,
        cost_estimate=pl.CostEstimate(flops=500_000_000, transcendentals=0, bytes_accessed=4_800_000),
        name="cut",
    )(weight)


def product(refs, weights, a, b):
    @pl.when(pl.program_id(0) == 0)
    def _():
        for i in range(4):
            b[384 * i : 384 * (i + 1), :] = weights[i][0]

    for i in range(12):
        a[:, HEAD * i : HEAD * (i + 1)] = refs[i][...].reshape(-1, HEAD)
    return jnp.dot(a[...], b[...], preferred_element_type=jnp.float32).reshape(-1, 8, 16, 384)


def project_kernel(*refs):
    out, a, b = refs[16:]
    out[...] = product(refs, refs[12:16], a, b).astype(out.dtype)


def project(rows, weights, half, side, dtype, steps=STEPS):
    size = 6 // steps
    specs = [
        pl.BlockSpec((size, 8, 16, HEAD), lambda i, f=steps * half * (r.shape[0] // 12): (f + i, 0, 0, 0))
        for r in rows
    ]
    return pl.pallas_call(
        project_kernel,
        grid=(steps,),
        in_specs=specs + [pl.BlockSpec((1, 384, 384), lambda i: (side, 0, 0))] * 4,
        out_specs=pl.BlockSpec((size, 8, 16, 384), lambda i: (i, 0, 0, 0)),
        out_shape=jax.ShapeDtypeStruct((6, 8, 16, 384), dtype),
        scratch_shapes=[pltpu.VMEM((128 * size, 1536), jnp.bfloat16), pltpu.VMEM((1536, 384), jnp.bfloat16)],
        cost_estimate=pl.CostEstimate(flops=1_000_000_000, transcendentals=0, bytes_accessed=4_500_000),
        name="project",
    )(*rows, *weights)


def hd_pairs(step, planes=0):
    return [
        (4 * z + x, 4 * ((z + planes) % 2) + (x + step) % 4) for z in range(2) for x in range(4)
    ]


def place():
    return lax.axis_index("ha"), lax.axis_index("wa"), lax.axis_size("ha"), lax.axis_size("wa")


def shards(queries, video_keys, video_values, text_keys, text_values, tile_radius, out_weight):
    n_frames = queries.shape[0]
    n_ha = lax.axis_size("ha")
    n_wa = lax.axis_size("wa")
    ring = [(i, (i + 1) % n_wa) for i in range(n_wa)]
    back = [(t, s) for s, t in ring]
    partner = [(i, i + 1 if i % 2 == 0 else i - 1) for i in range(n_ha)]
    chips = [(i, (i + 2) % n_ha) for i in range(n_ha)]
    turn = [
        (i * n_wa + s, i * n_wa + t)
        for i in range(n_ha)
        for s, t in (ring if i % 2 else back)
    ]

    def swap(piece):
        return lax.ppermute(piece, "ha", partner)

    windows = []
    for first, count in GROUPS:
        low, high = pack(video_keys, video_values, first, count)
        from_left = lax.ppermute(high, "wa", ring)
        from_right = lax.ppermute(low, "wa", back)
        partner_low, partner_high = swap(low), swap(high)
        picked = choose(low, high, partner_low, partner_high)
        over = lax.ppermute(picked, "ha", chips)
        corner = lax.ppermute(over, ("ha", "wa"), turn)
        window = (low, high, partner_low, partner_high, over, swap(over),
                  from_left, from_right, swap(from_left), swap(from_right),
                  corner, swap(corner))
        windows += [(window, i) for i in range(count)]
    pieces = cut(out_weight)
    weights = [
        pieces[0],
        lax.ppermute(pieces[1], "hd", hd_pairs(1)),
        lax.ppermute(pieces[2], "hd", hd_pairs(-1)),
        lax.ppermute(pieces[3], "hd", hd_pairs(2)),
    ]
    def spread(piece):
        return [
            piece,
            lax.ppermute(piece, "hd", hd_pairs(1)),
            lax.ppermute(piece, "hd", hd_pairs(-1)),
            lax.ppermute(piece, "hd", hd_pairs(2)),
        ]

    def head(h, times, split):
        window, sub = windows[h]
        return attend(tile_radius, queries, text_keys, text_values, window, h, sub, place, times, split)

    (first_head,) = head(0, (0, 1), False)
    (second_head,) = head(1, (0, 1), False)
    halves = head(2, (0, 1), True)
    last = {t: spread(halves[t]) for t in (1, 0)}
    gathered = [[spread(first_head)] * 2, [spread(second_head)] * 2, [last[0], last[1]]]
    lines = [[gathered[h][t][g] for g in range(4) for h in range(3)] for t in range(2)]
    arrived = {}
    for t in (1, 0):
        other = project(lines[t], weights, t, 1, jnp.bfloat16)
        arrived[t] = lax.ppermute(other, "hd", hd_pairs(0, 1))
    done = {}
    for t in (1, 0):
        mine = project(lines[t], weights, t, 0, jnp.float32)
        done[t] = (mine + arrived[t].astype(jnp.float32)).astype(jnp.bfloat16)
    out = jnp.pad(done[1], ((n_frames // 2, 0), (0, 0), (0, 0), (0, 0)))
    return lax.dynamic_update_slice(out, done[0], (0, 0, 0, 0))


def solution(mesh):
    placed = (
        P(None, "ha", "wa", "hd"),
        P(None, "ha", "wa", "hd"),
        P(None, "ha", "wa", "hd"),
        P(None, "hd"),
        P(None, "hd"),
        P(None, None, "ha", "wa"),
        P("hd", None),
    )
    return jax.shard_map(
        shards, mesh=mesh, in_specs=placed, out_specs=P(None, "ha", "wa", "hd"), check_vma=False
    )
```

```python
import functools
import jax
import jax.numpy as jnp
from jax import lax
from jax.experimental import pallas as pl
from jax.experimental.pallas import tpu as pltpu
from jax.sharding import PartitionSpec as P

HEAD=128; LIMIT=64.0
SCALE = 1.4426950408889634 * HEAD ** -0.5
NT=(((1,),(1,)),((),()))


def attend_kernel(rad, q, tk, tv, *refs, n_seg, coords, sub, times, split, QB, KW):
    segs = refs[:n_seg]
    qs, kbuf, vbuf, tvb, mref, peak, acc, lst, cnt, sems = refs[-10:]
    out = refs[n_seg:-10]
    tiles = [(t, e) for t in times for e in range(2)]
    base = 6 * times[0]
    ha, wa, n_ha, n_wa = coords()
    copies=[]
    for i,s in enumerate(segs):
        copies.append(pltpu.make_async_copy(s.at[sub,0], kbuf.at[i], sems.at[2*i]))
        copies.append(pltpu.make_async_copy(s.at[sub,1], vbuf.at[i,:,pl.ds(0,128)], sems.at[2*i+1]))
    for c in copies: c.start()
    is_odd = ha % 2
    across_ok = jnp.where(is_odd==1, ha + 1 < n_ha, ha > 0).astype(jnp.int32)
    left_ok = (wa>0).astype(jnp.int32); right_ok=(wa+1<n_wa).astype(jnp.int32)
    rows=[0,0,1,1,2,2,0,0,1,1,2,2]
    cols=[0,1,0,1,0,1,-1,2,-1,2,-1,2]
    for qt, (t, e) in enumerate(tiles):
        r0=rad[0,t,0,e]; r1=rad[1,t,0,e]; r2=rad[2,t,0,e]
        row_ok=[1, (r1>=1).astype(jnp.int32), jnp.where(r1>=1, across_ok, 0)]
        n=jnp.int32(0)
        for s in range(12):
            gap=abs(cols[s]-e)
            if gap>1: continue
            ok=row_ok[rows[s]]
            if gap==1: ok=ok*(r2>=1).astype(jnp.int32)
            if cols[s]==-1: ok=ok*left_ok
            if cols[s]==2: ok=ok*right_ok
            place=s
            if s in (4,5): place=4+abs(s-4-is_odd)
            if s in (10,11): place=11-is_odd if s==10 else 10+is_odd
            lst[qt, n]=2*place+t
            n=n+ok
            lst[qt, n]=2*place+1-t
            n=n+ok*(r0>=1).astype(jnp.int32)
        cnt[qt]=n
    for qt, (t, e) in enumerate(tiles):
        f=6*t-base
        qs[qt]=q[f:f+6,:,8*e:8*e+8,:].reshape(384,HEAD)
    ones=jnp.ones((768,128),jnp.bfloat16)
    def fill(s,_):
        vbuf[s,:,128:256]=ones
        return 0
    lax.fori_loop(0,12,fill,0)
    tvb[:,0:128]=tv[...]
    tvb[:,128:256]=jnp.ones((256,128),jnp.bfloat16)

    def lanes_max(s):
        m=[s[:,128*j:128*j+128] for j in range(s.shape[1]//128)]
        while len(m)>1: m=[jnp.maximum(a,b) for a,b in zip(m[::2],m[1::2])]+([m[-1]] if len(m)%2 else [])
        return m[0]
    def bc(m, w):
        return jnp.concatenate([m]*(w//128),axis=1)
    def scores(qv,k):
        return lax.dot_general(qv,k,NT,preferred_element_type=jnp.float32)*SCALE
    def keys(code):
        return code//2, pl.ds(pl.multiple_of((code%2)*384,384),384)
    def text(qt,track):
        for r in range(0,384,QB):
            rs=pl.ds(r,QB)
            s=scores(qs[qt,rs,:],tk[...])
            if track:
                m=jnp.broadcast_to(jnp.max(s,axis=1,keepdims=True),(QB,128))
                mref[qt,rs,:]=m
                peak[qt,rs,:]=m
            else:
                m=mref[qt,rs,:]
            p=jnp.exp2(s-bc(m,256)).astype(jnp.bfloat16)
            acc[qt,rs,:]=jnp.dot(p,tvb[...],preferred_element_type=jnp.float32)
    def step(qt,codes):
        at=[keys(c) for c in codes]
        k=jnp.concatenate([kbuf[s,ks,:] for s,ks in at],axis=0)
        v=jnp.concatenate([vbuf[s,ks,:] for s,ks in at],axis=0)
        W=min(KW,k.shape[0]) if k.shape[0]%KW==0 else k.shape[0]
        parts=[(r,c) for r in range(0,384,QB) for c in range(0,k.shape[0],W)]
        def part(r,c): return scores(qs[qt,pl.ds(r,QB),:],k[c:c+W])
        nxt=part(*parts[0])
        for i,(r,c) in enumerate(parts):
            s=nxt
            if i+1<len(parts): nxt=part(*parts[i+1])
            rs=pl.ds(r,QB)
            peak[qt,rs,:]=jnp.maximum(peak[qt,rs,:],lanes_max(s))
            p=jnp.exp2(s-bc(mref[qt,rs,:],s.shape[1])).astype(jnp.bfloat16)
            acc[qt,rs,:]+=jnp.dot(p,v[c:c+W],preferred_element_type=jnp.float32)
    for qt in range(len(tiles)):
        text(qt,True)
    for c in copies: c.wait()
    def one(qt,_):
        n=cnt[qt]
        def quad(i,_):
            step(qt,[lst[qt,4*i+j] for j in range(4)])
            return 0
        lax.fori_loop(0,n//4,quad,0)
        m=n//4*4
        @pl.when(n%4>=2)
        def _():
            step(qt,(lst[qt,m],lst[qt,m+1]))
        @pl.when(n%2==1)
        def _():
            step(qt,(lst[qt,n-1],))
        return 0
    lax.fori_loop(0,len(tiles),one,0)
    gap=peak[0]-mref[0]
    for qt in range(1,len(tiles)): gap=jnp.maximum(gap,peak[qt]-mref[qt])
    @pl.when(jnp.max(gap)>LIMIT)
    def _():
        def redo(qt,_):
            text(qt,False)
            def safe(i,_):
                slot,ks=keys(lst[qt,i])
                def part(j,_):
                    rs=pl.ds(pl.multiple_of(j*128,128),128)
                    s=scores(qs[qt,rs,:],kbuf[slot,ks,:])
                    old=mref[qt,rs,:]
                    new=jnp.maximum(old,jnp.broadcast_to(jnp.max(s,axis=1,keepdims=True),(128,128)))
                    mref[qt,rs,:]=new
                    p=jnp.exp2(s-bc(new,384)).astype(jnp.bfloat16)
                    acc[qt,rs,:]=acc[qt,rs,:]*bc(jnp.exp2(old-new),256)+jnp.dot(p,vbuf[slot,ks,:],preferred_element_type=jnp.float32)
                    return 0
                return lax.fori_loop(0,3,part,0)
            return lax.fori_loop(0,cnt[qt],safe,0)
        lax.fori_loop(0,len(tiles),redo,0)
    for qt, (t, e) in enumerate(tiles):
        ref=out[times.index(t) if split else 0]
        f=0 if split else 6*t-base
        ref[f:f+6,:,8*e:8*e+8,:]=(acc[qt,:,0:128]/acc[qt,:,128:256]).astype(jnp.bfloat16).reshape(6,8,8,HEAD)


def attend(rad,q,tk,tv,segs,h,sub,coords,times=(0,1),split=True,QB=192,KW=768):
    n=len(segs); nt=2*len(times); frames=6*len(times)
    first=times[0] if len(times)==1 else 0
    size=6 if split else frames
    return pl.pallas_call(
        functools.partial(attend_kernel,n_seg=n,coords=coords,sub=sub,times=times,split=split,QB=QB,KW=KW),
        grid=(1,),
        in_specs=[pl.BlockSpec(memory_space=pltpu.SMEM),
            pl.BlockSpec((frames,8,16,HEAD),lambda i:(first,0,0,h)),
            pl.BlockSpec((256,HEAD),lambda i:(0,h)),
            pl.BlockSpec((256,HEAD),lambda i:(0,h))]+[pl.BlockSpec(memory_space=pltpu.HBM)]*n,
        out_specs=[pl.BlockSpec((size,8,16,HEAD),lambda i:(0,0,0,0))]*(frames//size),
        out_shape=[jax.ShapeDtypeStruct((size,8,16,HEAD),jnp.bfloat16)]*(frames//size),
        scratch_shapes=[pltpu.VMEM((nt,384,HEAD),jnp.bfloat16),pltpu.VMEM((12,768,HEAD),jnp.bfloat16),
            pltpu.VMEM((12,768,256),jnp.bfloat16),pltpu.VMEM((256,256),jnp.bfloat16),
            pltpu.VMEM((nt,384,128),jnp.float32),pltpu.VMEM((nt,384,128),jnp.float32),pltpu.VMEM((nt,384,256),jnp.float32),
            pltpu.SMEM((nt,32),jnp.int32),pltpu.SMEM((nt,),jnp.int32),pltpu.SemaphoreType.DMA((2*n,))],
        cost_estimate=pl.CostEstimate(flops=3_000_000_000*len(times),transcendentals=6_000_000,bytes_accessed=6_000_000),
        name="attend",
    )(rad,q,tk,tv,*segs)


GROUPS = ((0, 1), (1, 2))
STEPS = 1


def pack_kernel(*refs):
    low, high = refs[-2:]
    for i in range(low.shape[0]):
        for col, ref in enumerate((low, high)):
            for j in range(2):
                ref[i, j] = refs[2 * i + j][:, :, 8 * col : 8 * col + 8, :]


def pack(keys, values, first, count):
    specs = [
        pl.BlockSpec((12, 8, 16, HEAD), lambda i, h=h: (0, 0, 0, h))
        for h in range(first, first + count)
        for _ in range(2)
    ]
    shape = (count, 2, 12, 8, 8, HEAD)
    outs = pl.pallas_call(
        pack_kernel,
        grid=(1,),
        in_specs=specs,
        out_specs=[pl.BlockSpec(shape, lambda i: (0,) * 6)] * 2,
        out_shape=[jax.ShapeDtypeStruct(shape, jnp.bfloat16)] * 2,
        cost_estimate=pl.CostEstimate(flops=500_000_000, transcendentals=0, bytes_accessed=1_600_000),
        name="pack",
    )(*[keys, values] * count)
    return [out.reshape(count, 2, 768, HEAD) for out in outs]


def choose_kernel(own_low, own_high, partner_low, partner_high, out, sem):
    ha = lax.axis_index("ha")
    inner = (ha > 0) & (ha + 1 < lax.axis_size("ha"))
    odd = ha % 2 == 1
    for is_inner, refs in ((True, (own_low, own_high)), (False, (partner_low, partner_high))):
        for is_odd, ref in enumerate(refs):

            @pl.when((inner == is_inner) & (odd == bool(is_odd)))
            def _():
                copy = pltpu.make_async_copy(ref, out, sem)
                copy.start()
                copy.wait()


def choose(*pieces):
    return pl.pallas_call(
        choose_kernel,
        in_specs=[pl.BlockSpec(memory_space=pltpu.HBM)] * 4,
        out_shape=jax.ShapeDtypeStruct(pieces[0].shape, jnp.bfloat16),
        scratch_shapes=[pltpu.SemaphoreType.DMA],
        cost_estimate=pl.CostEstimate(flops=200_000_000, transcendentals=0, bytes_accessed=800_000),
        name="choose",
    )(*pieces)


def cut_kernel(w, own, plus, minus, far):
    hd = lax.axis_index("hd")
    x = hd % 4
    plane = hd // 4
    for ref, step in ((own, 0), (plus, 1), (minus, 3), (far, 2)):
        for j in range(2):
            col = (x + step) % 4 + 4 * ((plane + j) % 2)
            ref[j] = w[:, pl.ds(pl.multiple_of(col * 384, 384), 384)]


def cut(weight):
    return pl.pallas_call(
        cut_kernel,
        out_shape=[jax.ShapeDtypeStruct((2, 384, 384), jnp.bfloat16)] * 4,
        cost_estimate=pl.CostEstimate(flops=500_000_000, transcendentals=0, bytes_accessed=4_800_000),
        name="cut",
    )(weight)


def product(refs, weights, a, b):
    @pl.when(pl.program_id(0) == 0)
    def _():
        for i in range(4):
            b[384 * i : 384 * (i + 1), :] = weights[i][0]

    for i in range(12):
        a[:, HEAD * i : HEAD * (i + 1)] = refs[i][...].reshape(-1, HEAD)
    return jnp.dot(a[...], b[...], preferred_element_type=jnp.float32).reshape(-1, 8, 16, 384)


def project_kernel(*refs):
    out, a, b = refs[16:]
    out[...] = product(refs, refs[12:16], a, b).astype(out.dtype)


def project(rows, weights, half, side, dtype, steps=STEPS):
    size = 6 // steps
    specs = [
        pl.BlockSpec((size, 8, 16, HEAD), lambda i, f=steps * half * (r.shape[0] // 12): (f + i, 0, 0, 0))
        for r in rows
    ]
    return pl.pallas_call(
        project_kernel,
        grid=(steps,),
        in_specs=specs + [pl.BlockSpec((1, 384, 384), lambda i: (side, 0, 0))] * 4,
        out_specs=pl.BlockSpec((size, 8, 16, 384), lambda i: (i, 0, 0, 0)),
        out_shape=jax.ShapeDtypeStruct((6, 8, 16, 384), dtype),
        scratch_shapes=[pltpu.VMEM((128 * size, 1536), jnp.bfloat16), pltpu.VMEM((1536, 384), jnp.bfloat16)],
        cost_estimate=pl.CostEstimate(flops=1_000_000_000, transcendentals=0, bytes_accessed=4_500_000),
        name="project",
    )(*rows, *weights)


def hd_pairs(step, planes=0):
    return [
        (4 * z + x, 4 * ((z + planes) % 2) + (x + step) % 4) for z in range(2) for x in range(4)
    ]


def place():
    return lax.axis_index("ha"), lax.axis_index("wa"), lax.axis_size("ha"), lax.axis_size("wa")


def shards(queries, video_keys, video_values, text_keys, text_values, tile_radius, out_weight):
    n_frames = queries.shape[0]
    n_ha = lax.axis_size("ha")
    n_wa = lax.axis_size("wa")
    ring = [(i, (i + 1) % n_wa) for i in range(n_wa)]
    back = [(t, s) for s, t in ring]
    partner = [(i, i + 1 if i % 2 == 0 else i - 1) for i in range(n_ha)]
    chips = [(i, (i + 2) % n_ha) for i in range(n_ha)]
    turn = [
        (i * n_wa + s, i * n_wa + t)
        for i in range(n_ha)
        for s, t in (ring if i % 2 else back)
    ]

    def swap(piece):
        return lax.ppermute(piece, "ha", partner)

    windows = []
    for first, count in GROUPS:
        low, high = pack(video_keys, video_values, first, count)
        from_left = lax.ppermute(high, "wa", ring)
        from_right = lax.ppermute(low, "wa", back)
        partner_low, partner_high = swap(low), swap(high)
        picked = choose(low, high, partner_low, partner_high)
        over = lax.ppermute(picked, "ha", chips)
        corner = lax.ppermute(over, ("ha", "wa"), turn)
        window = (low, high, partner_low, partner_high, over, swap(over),
                  from_left, from_right, swap(from_left), swap(from_right),
                  corner, swap(corner))
        windows += [(window, i) for i in range(count)]
    pieces = cut(out_weight)
    weights = [
        pieces[0],
        lax.ppermute(pieces[1], "hd", hd_pairs(1)),
        lax.ppermute(pieces[2], "hd", hd_pairs(-1)),
        lax.ppermute(pieces[3], "hd", hd_pairs(2)),
    ]
    def spread(piece):
        return [
            piece,
            lax.ppermute(piece, "hd", hd_pairs(1)),
            lax.ppermute(piece, "hd", hd_pairs(-1)),
            lax.ppermute(piece, "hd", hd_pairs(2)),
        ]

    def head(h, times, split):
        window, sub = windows[h]
        return attend(tile_radius, queries, text_keys, text_values, window, h, sub, place, times, split)

    (first_head,) = head(0, (0, 1), False)
    (second_head,) = head(1, (0, 1), False)
    halves = head(2, (0, 1), True)
    last = {t: spread(halves[t]) for t in (1, 0)}
    gathered = [[spread(first_head)] * 2, [spread(second_head)] * 2, [last[0], last[1]]]
    lines = [[gathered[h][t][g] for g in range(4) for h in range(3)] for t in range(2)]
    arrived = {}
    for t in (1, 0):
        other = project(lines[t], weights, t, 1, jnp.bfloat16)
        arrived[t] = lax.ppermute(other, "hd", hd_pairs(0, 1))
    done = {}
    for t in (1, 0):
        mine = project(lines[t], weights, t, 0, jnp.float32)
        done[t] = (mine + arrived[t].astype(jnp.float32)).astype(jnp.bfloat16)
    out = jnp.pad(done[1], ((n_frames // 2, 0), (0, 0), (0, 0), (0, 0)))
    return lax.dynamic_update_slice(out, done[0], (0, 0, 0, 0))


def solution(mesh):
    placed = (
        P(None, "ha", "wa", "hd"),
        P(None, "ha", "wa", "hd"),
        P(None, "ha", "wa", "hd"),
        P(None, "hd"),
        P(None, "hd"),
        P(None, None, "ha", "wa"),
        P("hd", None),
    )
    return jax.shard_map(
        shards, mesh=mesh, in_specs=placed, out_specs=P(None, "ha", "wa", "hd"), check_vma=False
    )
```

```python
import functools
import jax
import jax.numpy as jnp
from jax import lax
from jax.experimental import pallas as pl
from jax.experimental.pallas import tpu as pltpu
from jax.sharding import PartitionSpec as P

HEAD=128; LIMIT=64.0
SCALE = 1.4426950408889634 * HEAD ** -0.5
NT=(((1,),(1,)),((),()))


def attend_kernel(rad, q, tk, tv, *refs, n_seg, coords, subs, times, split, QB, KW):
    segs = refs[:n_seg]
    qs, kbuf, vbuf, tvb, mref, peak, acc, lst, cnt, sems = refs[-10:]
    out = refs[n_seg:-10]
    tiles = [(t, e) for t in times for e in range(2)]
    base = 6 * times[0]
    ha, wa, n_ha, n_wa = coords()
    copies=[]
    for i,s in enumerate(segs):
        copies.append(pltpu.make_async_copy(s.at[subs[i],0], kbuf.at[i], sems.at[2*i]))
        copies.append(pltpu.make_async_copy(s.at[subs[i],1], vbuf.at[i,:,pl.ds(0,128)], sems.at[2*i+1]))
    for c in copies: c.start()
    is_odd = ha % 2
    across_ok = jnp.where(is_odd==1, ha + 1 < n_ha, ha > 0).astype(jnp.int32)
    left_ok = (wa>0).astype(jnp.int32); right_ok=(wa+1<n_wa).astype(jnp.int32)
    rows=[0,0,1,1,2,2,0,0,1,1,2,2]
    cols=[0,1,0,1,0,1,-1,2,-1,2,-1,2]
    for qt, (t, e) in enumerate(tiles):
        r0=rad[0,t,0,e]; r1=rad[1,t,0,e]; r2=rad[2,t,0,e]
        row_ok=[1, (r1>=1).astype(jnp.int32), jnp.where(r1>=1, across_ok, 0)]
        n=jnp.int32(0)
        for s in range(12):
            gap=abs(cols[s]-e)
            if gap>1: continue
            ok=row_ok[rows[s]]
            if gap==1: ok=ok*(r2>=1).astype(jnp.int32)
            if cols[s]==-1: ok=ok*left_ok
            if cols[s]==2: ok=ok*right_ok
            place=s
            if s in (4,5): place=4+abs(s-4-is_odd)
            if s in (10,11): place=11-is_odd if s==10 else 10+is_odd
            lst[qt, n]=2*place+t
            n=n+ok
            lst[qt, n]=2*place+1-t
            n=n+ok*(r0>=1).astype(jnp.int32)
        cnt[qt]=n
    for qt, (t, e) in enumerate(tiles):
        f=6*t-base
        qs[qt]=q[f:f+6,:,8*e:8*e+8,:].reshape(384,HEAD)
    ones=jnp.ones((768,128),jnp.bfloat16)
    def fill(s,_):
        vbuf[s,:,128:256]=ones
        return 0
    lax.fori_loop(0,12,fill,0)
    tvb[:,0:128]=tv[...]
    tvb[:,128:256]=jnp.ones((256,128),jnp.bfloat16)

    def lanes_max(s):
        m=[s[:,128*j:128*j+128] for j in range(s.shape[1]//128)]
        while len(m)>1: m=[jnp.maximum(a,b) for a,b in zip(m[::2],m[1::2])]+([m[-1]] if len(m)%2 else [])
        return m[0]
    def bc(m, w):
        return jnp.concatenate([m]*(w//128),axis=1)
    def scores(qv,k):
        return lax.dot_general(qv,k,NT,preferred_element_type=jnp.float32)*SCALE
    def keys(code):
        return code//2, pl.ds(pl.multiple_of((code%2)*384,384),384)
    def text(qt,track):
        for r in range(0,384,QB):
            rs=pl.ds(r,QB)
            s=scores(qs[qt,rs,:],tk[...])
            if track:
                m=jnp.broadcast_to(jnp.max(s,axis=1,keepdims=True),(QB,128))
                mref[qt,rs,:]=m
                peak[qt,rs,:]=m
            else:
                m=mref[qt,rs,:]
            p=jnp.exp2(s-bc(m,256)).astype(jnp.bfloat16)
            acc[qt,rs,:]=jnp.dot(p,tvb[...],preferred_element_type=jnp.float32)
    def step(qt,codes):
        at=[keys(c) for c in codes]
        k=jnp.concatenate([kbuf[s,ks,:] for s,ks in at],axis=0)
        v=jnp.concatenate([vbuf[s,ks,:] for s,ks in at],axis=0)
        W=min(KW,k.shape[0]) if k.shape[0]%KW==0 else k.shape[0]
        parts=[(r,c) for r in range(0,384,QB) for c in range(0,k.shape[0],W)]
        def part(r,c): return scores(qs[qt,pl.ds(r,QB),:],k[c:c+W])
        nxt=part(*parts[0])
        for i,(r,c) in enumerate(parts):
            s=nxt
            if i+1<len(parts): nxt=part(*parts[i+1])
            rs=pl.ds(r,QB)
            peak[qt,rs,:]=jnp.maximum(peak[qt,rs,:],lanes_max(s))
            p=jnp.exp2(s-bc(mref[qt,rs,:],s.shape[1])).astype(jnp.bfloat16)
            acc[qt,rs,:]+=jnp.dot(p,v[c:c+W],preferred_element_type=jnp.float32)
    for qt in range(len(tiles)):
        text(qt,True)
    for c in copies: c.wait()
    def one(qt,_):
        n=cnt[qt]
        def quad(i,_):
            step(qt,[lst[qt,4*i+j] for j in range(4)])
            return 0
        lax.fori_loop(0,n//4,quad,0)
        m=n//4*4
        @pl.when(n%4>=2)
        def _():
            step(qt,(lst[qt,m],lst[qt,m+1]))
        @pl.when(n%2==1)
        def _():
            step(qt,(lst[qt,n-1],))
        return 0
    lax.fori_loop(0,len(tiles),one,0)
    gap=peak[0]-mref[0]
    for qt in range(1,len(tiles)): gap=jnp.maximum(gap,peak[qt]-mref[qt])
    @pl.when(jnp.max(gap)>LIMIT)
    def _():
        def redo(qt,_):
            text(qt,False)
            def safe(i,_):
                slot,ks=keys(lst[qt,i])
                def part(j,_):
                    rs=pl.ds(pl.multiple_of(j*128,128),128)
                    s=scores(qs[qt,rs,:],kbuf[slot,ks,:])
                    old=mref[qt,rs,:]
                    new=jnp.maximum(old,jnp.broadcast_to(jnp.max(s,axis=1,keepdims=True),(128,128)))
                    mref[qt,rs,:]=new
                    p=jnp.exp2(s-bc(new,384)).astype(jnp.bfloat16)
                    acc[qt,rs,:]=acc[qt,rs,:]*bc(jnp.exp2(old-new),256)+jnp.dot(p,vbuf[slot,ks,:],preferred_element_type=jnp.float32)
                    return 0
                return lax.fori_loop(0,3,part,0)
            return lax.fori_loop(0,cnt[qt],safe,0)
        lax.fori_loop(0,len(tiles),redo,0)
    for qt, (t, e) in enumerate(tiles):
        ref=out[times.index(t) if split else 0]
        f=0 if split else 6*t-base
        ref[f:f+6,:,8*e:8*e+8,:]=(acc[qt,:,0:128]/acc[qt,:,128:256]).astype(jnp.bfloat16).reshape(6,8,8,HEAD)


def attend(rad,q,tk,tv,segs,h,subs,coords,times=(0,1),split=True,QB=192,KW=768):
    n=len(segs); nt=2*len(times); frames=6*len(times)
    first=times[0] if len(times)==1 else 0
    size=6 if split else frames
    return pl.pallas_call(
        functools.partial(attend_kernel,n_seg=n,coords=coords,subs=subs,times=times,split=split,QB=QB,KW=KW),
        grid=(1,),
        in_specs=[pl.BlockSpec(memory_space=pltpu.SMEM),
            pl.BlockSpec((frames,8,16,HEAD),lambda i:(first,0,0,h)),
            pl.BlockSpec((256,HEAD),lambda i:(0,h)),
            pl.BlockSpec((256,HEAD),lambda i:(0,h))]+[pl.BlockSpec(memory_space=pltpu.HBM)]*n,
        out_specs=[pl.BlockSpec((size,8,16,HEAD),lambda i:(0,0,0,0))]*(frames//size),
        out_shape=[jax.ShapeDtypeStruct((size,8,16,HEAD),jnp.bfloat16)]*(frames//size),
        scratch_shapes=[pltpu.VMEM((nt,384,HEAD),jnp.bfloat16),pltpu.VMEM((12,768,HEAD),jnp.bfloat16),
            pltpu.VMEM((12,768,256),jnp.bfloat16),pltpu.VMEM((256,256),jnp.bfloat16),
            pltpu.VMEM((nt,384,128),jnp.float32),pltpu.VMEM((nt,384,128),jnp.float32),pltpu.VMEM((nt,384,256),jnp.float32),
            pltpu.SMEM((nt,32),jnp.int32),pltpu.SMEM((nt,),jnp.int32),pltpu.SemaphoreType.DMA((2*n,))],
        cost_estimate=pl.CostEstimate(flops=3_000_000_000*len(times),transcendentals=6_000_000,bytes_accessed=6_000_000),
        name="attend",
    )(rad,q,tk,tv,*segs)


GROUPS = ((0, 1), (1, 2))
STEPS = 1


def pack_kernel(*refs):
    count = len(refs) // 4
    for i in range(count):
        for col in range(2):
            for j in range(2):
                refs[2 * count + 2 * i + col][0, j] = refs[2 * i + j][:, :, 8 * col : 8 * col + 8, :]


def pack(keys, values, first, count):
    specs = [
        pl.BlockSpec((12, 8, 16, HEAD), lambda i, h=h: (0, 0, 0, h))
        for h in range(first, first + count)
        for _ in range(2)
    ]
    shape = (1, 2, 12, 8, 8, HEAD)
    outs = pl.pallas_call(
        pack_kernel,
        grid=(1,),
        in_specs=specs,
        out_specs=[pl.BlockSpec(shape, lambda i: (0,) * 6)] * (2 * count),
        out_shape=[jax.ShapeDtypeStruct(shape, jnp.bfloat16)] * (2 * count),
        cost_estimate=pl.CostEstimate(flops=500_000_000, transcendentals=0, bytes_accessed=1_600_000),
        name="pack",
    )(*[keys, values] * count)
    return [out.reshape(1, 2, 768, HEAD) for out in outs]


def choose_kernel(*refs):
    count = (len(refs) - 2) // 4
    out, sem = refs[-2:]
    ha = lax.axis_index("ha")
    inner = (ha > 0) & (ha + 1 < lax.axis_size("ha"))
    odd = ha % 2 == 1
    for source in range(4):

        @pl.when((inner == (source < 2)) & (odd == (source % 2 == 1)))
        def _():
            copies = [
                pltpu.make_async_copy(refs[4 * i + source].at[0], out.at[i], sem.at[i])
                for i in range(count)
            ]
            for copy in copies:
                copy.start()
            for copy in copies:
                copy.wait()


def choose(*pieces):
    count = len(pieces) // 4
    return pl.pallas_call(
        choose_kernel,
        in_specs=[pl.BlockSpec(memory_space=pltpu.HBM)] * len(pieces),
        out_shape=jax.ShapeDtypeStruct((count, *pieces[0].shape[1:]), jnp.bfloat16),
        scratch_shapes=[pltpu.SemaphoreType.DMA((count,))],
        cost_estimate=pl.CostEstimate(flops=200_000_000, transcendentals=0, bytes_accessed=800_000),
        name="choose",
    )(*pieces)


def cut_kernel(w, own, plus, minus, far):
    hd = lax.axis_index("hd")
    x = hd % 4
    plane = hd // 4
    for ref, step in ((own, 0), (plus, 1), (minus, 3), (far, 2)):
        for j in range(2):
            col = (x + step) % 4 + 4 * ((plane + j) % 2)
            ref[j] = w[:, pl.ds(pl.multiple_of(col * 384, 384), 384)]


def cut(weight):
    return pl.pallas_call(
        cut_kernel,
        out_shape=[jax.ShapeDtypeStruct((2, 384, 384), jnp.bfloat16)] * 4,
        cost_estimate=pl.CostEstimate(flops=500_000_000, transcendentals=0, bytes_accessed=4_800_000),
        name="cut",
    )(weight)


def product(refs, weights, a, b):
    @pl.when(pl.program_id(0) == 0)
    def _():
        for i in range(4):
            b[384 * i : 384 * (i + 1), :] = weights[i][0]

    for i in range(12):
        a[:, HEAD * i : HEAD * (i + 1)] = refs[i][...].reshape(-1, HEAD)
    return jnp.dot(a[...], b[...], preferred_element_type=jnp.float32).reshape(-1, 8, 16, 384)


def project_kernel(*refs):
    out, a, b = refs[16:]
    out[...] = product(refs, refs[12:16], a, b).astype(out.dtype)


def project(rows, weights, half, side, dtype, steps=STEPS):
    size = 6 // steps
    specs = [
        pl.BlockSpec((size, 8, 16, HEAD), lambda i, f=steps * half * (r.shape[0] // 12): (f + i, 0, 0, 0))
        for r in rows
    ]
    return pl.pallas_call(
        project_kernel,
        grid=(steps,),
        in_specs=specs + [pl.BlockSpec((1, 384, 384), lambda i: (side, 0, 0))] * 4,
        out_specs=pl.BlockSpec((size, 8, 16, 384), lambda i: (i, 0, 0, 0)),
        out_shape=jax.ShapeDtypeStruct((6, 8, 16, 384), dtype),
        scratch_shapes=[pltpu.VMEM((128 * size, 1536), jnp.bfloat16), pltpu.VMEM((1536, 384), jnp.bfloat16)],
        cost_estimate=pl.CostEstimate(flops=1_000_000_000, transcendentals=0, bytes_accessed=4_500_000),
        name="project",
    )(*rows, *weights)


def hd_pairs(step, planes=0):
    return [
        (4 * z + x, 4 * ((z + planes) % 2) + (x + step) % 4) for z in range(2) for x in range(4)
    ]


def place():
    return lax.axis_index("ha"), lax.axis_index("wa"), lax.axis_size("ha"), lax.axis_size("wa")


def shards(queries, video_keys, video_values, text_keys, text_values, tile_radius, out_weight):
    n_frames = queries.shape[0]
    n_ha = lax.axis_size("ha")
    n_wa = lax.axis_size("wa")
    ring = [(i, (i + 1) % n_wa) for i in range(n_wa)]
    back = [(t, s) for s, t in ring]
    partner = [(i, i + 1 if i % 2 == 0 else i - 1) for i in range(n_ha)]
    chips = [(i, (i + 2) % n_ha) for i in range(n_ha)]
    turn = [
        (i * n_wa + s, i * n_wa + t)
        for i in range(n_ha)
        for s, t in (ring if i % 2 else back)
    ]

    def swap(piece):
        return lax.ppermute(piece, "ha", partner)

    windows = []
    for first, count in GROUPS:
        own = pack(video_keys, video_values, first, count)
        near, picks = [], []
        for i in range(count):
            low, high = own[2 * i : 2 * i + 2]
            from_left = lax.ppermute(high, "wa", ring)
            from_right = lax.ppermute(low, "wa", back)
            partner_low, partner_high = swap(low), swap(high)
            picks += [low, high, partner_low, partner_high]
            near.append((low, high, partner_low, partner_high, from_left, from_right,
                         swap(from_left), swap(from_right)))
        picked = choose(*picks)
        over = lax.ppermute(picked, "ha", chips)
        corner = lax.ppermute(over, ("ha", "wa"), turn)
        far = (over, swap(over)), (corner, swap(corner))
        for i in range(count):
            windows.append(
                ((*near[i][:4], *far[0], *near[i][4:], *far[1]), (0,) * 4 + (i,) * 2 + (0,) * 4 + (i,) * 2)
            )
    pieces = cut(out_weight)
    weights = [
        pieces[0],
        lax.ppermute(pieces[1], "hd", hd_pairs(1)),
        lax.ppermute(pieces[2], "hd", hd_pairs(-1)),
        lax.ppermute(pieces[3], "hd", hd_pairs(2)),
    ]
    def spread(piece):
        return [
            piece,
            lax.ppermute(piece, "hd", hd_pairs(1)),
            lax.ppermute(piece, "hd", hd_pairs(-1)),
            lax.ppermute(piece, "hd", hd_pairs(2)),
        ]

    def head(h, times, split):
        window, subs = windows[h]
        return attend(tile_radius, queries, text_keys, text_values, window, h, subs, place, times, split)

    (first_head,) = head(0, (0, 1), False)
    (second_head,) = head(1, (0, 1), False)
    halves = head(2, (0, 1), True)
    last = {t: spread(halves[t]) for t in (1, 0)}
    gathered = [[spread(first_head)] * 2, [spread(second_head)] * 2, [last[0], last[1]]]
    lines = [[gathered[h][t][g] for g in range(4) for h in range(3)] for t in range(2)]
    arrived = {}
    for t in (1, 0):
        other = project(lines[t], weights, t, 1, jnp.bfloat16)
        arrived[t] = lax.ppermute(other, "hd", hd_pairs(0, 1))
    done = {}
    for t in (1, 0):
        mine = project(lines[t], weights, t, 0, jnp.float32)
        done[t] = (mine + arrived[t].astype(jnp.float32)).astype(jnp.bfloat16)
    out = jnp.pad(done[1], ((n_frames // 2, 0), (0, 0), (0, 0), (0, 0)))
    return lax.dynamic_update_slice(out, done[0], (0, 0, 0, 0))


def solution(mesh):
    placed = (
        P(None, "ha", "wa", "hd"),
        P(None, "ha", "wa", "hd"),
        P(None, "ha", "wa", "hd"),
        P(None, "hd"),
        P(None, "hd"),
        P(None, None, "ha", "wa"),
        P("hd", None),
    )
    return jax.shard_map(
        shards, mesh=mesh, in_specs=placed, out_specs=P(None, "ha", "wa", "hd"), check_vma=False
    )
```
